128 devices in a mesh: dp: 1, cp: 128 (over z, y, x, core).
Axes of the slice: x: 4, y: 4, z: 4, core: 2. Of those that a mesh axis runs over, the one named last changes fastest.
Arguments:
- latent: bfloat16 [512, 48, 96, 128], P(('dp', 'cp'))
- conv_kernels: bfloat16 [4, 3, 3, 3, 128, 128], replicated
- conv_biases: float32 [4, 128], replicated
- gn_gammas: float32 [4, 128], replicated
- gn_betas: float32 [4, 128], replicated
Outputs:
- output: bfloat16 [512, 48, 96, 128], P(('dp', 'cp'))
All inputs are finite; a program needn't handle non-finite values.
Results may differ from the reference program's by a relative error of at most 0.0138496.
Values are sent between devices in bfloat16 or wider.
A program may use at most 1 GiB of HBM per device.

```python
import jax
import jax.numpy as jnp
from jax import lax

FRAMES = 512
LAT_HEIGHT = 48
LAT_WIDTH = 96
CHANNELS = 128
GROUPS = 32
NORM_EPS = 1e-6


def setup_inputs(seed: int = 0, part: int = 0) -> dict:
    part_key = jax.random.fold_in(jax.random.key(seed), part)
    key_noise, key_slope, key_jitter, key_gain = jax.random.split(part_key, 4)
    key_kernel, key_bias, key_gamma, key_beta = jax.random.split(jax.random.key(seed + 1), 4)
    time_trend = jnp.linspace(-1.0, 1.0, FRAMES)
    chan_slope = jax.random.normal(key_slope, (CHANNELS,))
    frame_mean = time_trend[:, None] * chan_slope[None, :] + 0.3 * jax.random.normal(key_jitter, (FRAMES, CHANNELS))
    frame_gain = jnp.exp(0.5 * time_trend + 0.2 * jax.random.normal(key_gain, (FRAMES,)))
    base_noise = jax.random.normal(key_noise, (FRAMES, LAT_HEIGHT, LAT_WIDTH, CHANNELS))
    latent = base_noise * frame_gain[:, None, None, None] + frame_mean[:, None, None, :]
    conv_kernels = jax.random.normal(key_kernel, (4, 3, 3, 3, CHANNELS, CHANNELS)) * (27 * CHANNELS) ** -0.5
    conv_biases = 0.3 * jax.random.normal(key_bias, (4, CHANNELS))
    gn_gammas = 1.0 + 0.3 * jax.random.normal(key_gamma, (4, CHANNELS))
    gn_betas = 0.3 * jax.random.normal(key_beta, (4, CHANNELS))
    return {"latent": latent.astype(jnp.bfloat16), "conv_kernels": conv_kernels.astype(jnp.bfloat16), "conv_biases": conv_biases.astype(jnp.float32), "gn_gammas": gn_gammas.astype(jnp.float32), "gn_betas": gn_betas.astype(jnp.float32)}


def norm_act(hidden, gn_gamma, gn_beta):
    widened = hidden.astype(jnp.float32)
    grouped = widened.reshape(hidden.shape[:-1] + (GROUPS, CHANNELS // GROUPS))
    elem_count = grouped.size // GROUPS
    sum_one = jnp.sum(grouped, axis=(0, 1, 2, 4))
    sum_sq = jnp.sum(grouped * grouped, axis=(0, 1, 2, 4))
    grp_mean = sum_one / elem_count
    grp_var = sum_sq / elem_count - grp_mean * grp_mean
    normed = (grouped - grp_mean[:, None]) * lax.rsqrt(grp_var + NORM_EPS)[:, None]
    normed = (normed.reshape(hidden.shape) * gn_gamma + gn_beta).astype(jnp.bfloat16)
    return jax.nn.silu(normed.astype(jnp.float32)).astype(jnp.bfloat16)


def causal_conv(act_in, kernel, conv_bias):
    padded = jnp.concatenate([act_in[:1], act_in[:1], act_in], axis=0).astype(jnp.float32)
    result = lax.conv_general_dilated(padded[None], kernel.astype(jnp.float32), (1, 1, 1), ((0, 0), (1, 1), (1, 1)), dimension_numbers=("NDHWC", "DHWIO", "NDHWC"))[0]
    return (result + conv_bias).astype(jnp.bfloat16)


def reference(latent, conv_kernels, conv_biases, gn_gammas, gn_betas):
    def block_step(hidden, block_params):
        kernel_pair, bias_pair, gamma_pair, beta_pair = block_params
        inner = causal_conv(norm_act(hidden, gamma_pair[0], beta_pair[0]), kernel_pair[0], bias_pair[0])
        inner = causal_conv(norm_act(inner, gamma_pair[1], beta_pair[1]), kernel_pair[1], bias_pair[1])
        return (hidden.astype(jnp.float32) + inner.astype(jnp.float32)).astype(jnp.bfloat16), None

    block_params = (conv_kernels.reshape((2, 2) + conv_kernels.shape[1:]), conv_biases.reshape(2, 2, CHANNELS), gn_gammas.reshape(2, 2, CHANNELS), gn_betas.reshape(2, 2, CHANNELS))
    decoded, _ = lax.scan(block_step, latent, block_params)
    return decoded
```

```python
import functools

import jax
import jax.numpy as jnp
from jax import lax
from jax.experimental import pallas as pl
from jax.experimental.pallas import tpu as pltpu
from jax.sharding import PartitionSpec as P

GROUP_WIDTH = 4
NORM_EPS = 1e-6
LAYERS = 4
NEAR = 8
ROWS = 6
UNROLL = 2
MESH = pl.DeviceIdType.MESH
BF16 = jnp.bfloat16
F32 = jnp.float32


def _plan():
    plan = []
    for out in range(2):
        pieces = [(out + k, di, ((k, di, 0), (k, di, 1))) for di in range(3) for k in range(3)]
        plan.append(pieces)
    pieces = []
    for di in range(3):
        for f in range(4):
            pieces.append((f, di, ((f, di, 2) if f < 3 else None, (f - 1, di, 2) if f > 0 else None)))
    plan.append(pieces)
    return plan


PLAN = _plan()


def kernel(n_dev, *refs):
    (lat, kern, bias, gamma, beta, out, cur, mid, act, halo, wts, part1, part2, gat1, gat2, coef, mid_sum, left_sum, right_sum, load_sem, wts_sem, out_sem, halo_send, halo_recv, send1, recv1, send2, recv2) = refs
    n_frames, height, width, chans = lat.shape
    far = n_dev // NEAR
    elem_count = float(n_dev * n_frames * height * width * GROUP_WIDTH)
    me = lax.axis_index("cp")
    near_pos = lax.rem(me, NEAR)
    far_pos = me // NEAR
    near_base = me - near_pos

    def near_peer(j):
        slot = lax.rem(near_pos + j, NEAR)
        return slot, near_base + slot

    def far_peer(j):
        slot = lax.rem(far_pos + j, far)
        return slot, slot * NEAR + near_pos

    barrier = pltpu.get_barrier_semaphore()
    for j in range(1, NEAR):
        pl.semaphore_signal(barrier, inc=1, device_id={"cp": near_peer(j)[1]}, device_id_type=MESH)
    for j in range(1, far):
        pl.semaphore_signal(barrier, inc=1, device_id={"cp": far_peer(j)[1]}, device_id_type=MESH)

    for device in (lax.rem(me + 1, n_dev), lax.rem(me + n_dev - 1, n_dev)):
        pl.semaphore_signal(barrier, inc=1, device_id={"cp": device}, device_id_type=MESH)

    frame_loads = [pltpu.make_async_copy(lat.at[f], cur.at[f], load_sem.at[f]) for f in range(n_frames)]
    for copy in frame_loads:
        copy.start()
    wts_loads = [pltpu.make_async_copy(kern.at[n], wts.at[n], wts_sem.at[n]) for n in range(LAYERS)]
    for copy in wts_loads:
        copy.start()

    pl.semaphore_wait(barrier, NEAR - 1 + far - 1 + 2)

    def halo_copy(src, slot):
        return pltpu.make_async_remote_copy(src_ref=src.at[pl.ds(n_frames - 2, 2)], dst_ref=halo.at[slot], send_sem=halo_send.at[slot], recv_sem=halo_recv.at[slot], device_id={"cp": me + 1}, device_id_type=MESH)

    @pl.when(me < n_dev - 1)
    def _():
        halo_copy(lat, 0).start()

    zero_row = jnp.zeros((width, chans), BF16)
    for f in range(n_frames + 2):
        act[f, 0] = zero_row
        act[f, height + 1] = zero_row
    edge = jnp.zeros((8, chans), F32)
    for r in range(ROWS):
        for o in range(2):
            left_sum[r, o, pl.ds(0, 8), :] = edge
            right_sum[r, o, pl.ds(width + 8, 8), :] = edge

    def row_sums(value):
        parts = value.reshape(width // 8, 8, chans)
        return jnp.sum(parts, axis=0), jnp.sum(parts * parts, axis=0)

    zero_sums = (jnp.zeros((8, chans), F32), jnp.zeros((8, chans), F32))

    def latent_sums(f, sums):
        def step(i, sums):
            for r in range(2):
                s1, s2 = row_sums(cur[f, 2 * i + r].astype(F32))
                sums = (sums[0] + s1, sums[1] + s2)
            return sums

        return lax.fori_loop(0, height // 2, step, sums)

    def group_total(sums):
        lane = lax.broadcasted_iota(jnp.int32, sums.shape, 1)
        for d in (1, 2):
            other = jnp.where(lax.rem(lane, 2 * d) < d, pltpu.roll(sums, chans - d, axis=1), pltpu.roll(sums, d, axis=1))
            sums = sums + other
        return sums

    def exchange(layer, size, pos, peer, part, gat, send, recv):
        def copy(j):
            slot, device = peer(j)
            return pltpu.make_async_remote_copy(src_ref=part, dst_ref=gat.at[layer, pos], send_sem=send.at[j], recv_sem=recv.at[layer, pos], device_id={"cp": device}, device_id_type=MESH)

        for j in range(1, size):
            copy(j).start()
        gat[layer, pos] = part[...]
        for j in range(1, size):
            slot, device = peer(j)
            pltpu.make_async_remote_copy(src_ref=part, dst_ref=gat.at[layer, slot], send_sem=send.at[j], recv_sem=recv.at[layer, slot], device_id={"cp": device}, device_id_type=MESH).wait_recv()
        total = gat[layer, 0]
        for slot in range(1, size):
            total = total + gat[layer, slot]
        for j in range(1, size):
            copy(j).wait_send()
        return total

    def norm_coefs(layer, sums):
        part1[...] = jnp.concatenate([jnp.sum(sums[0], axis=0, keepdims=True), jnp.sum(sums[1], axis=0, keepdims=True)], axis=0)
        part2[...] = exchange(layer, NEAR, near_pos, near_peer, part1, gat1, send1, recv1)
        total = exchange(layer, far, far_pos, far_peer, part2, gat2, send2, recv2)
        total = group_total(total)
        mean = total[0:1] / elem_count
        var = total[1:2] / elem_count - mean * mean
        scale = lax.rsqrt(var + NORM_EPS) * gamma[layer]
        coef[0] = scale
        coef[1] = beta[layer] - mean * scale

    def act_rows(value):
        normed = (value.astype(F32) * coef[0] + coef[1]).astype(BF16).astype(F32)
        half = normed * 0.5
        return (half + half * jnp.tanh(half)).astype(BF16)

    def act_frames(src, frames, first):
        def step(i, carry):
            for f in frames:
                for r in range(2):
                    act[first + f, 2 * i + r + 1] = act_rows(src[f, 2 * i + r])
            return carry

        lax.fori_loop(0, height // 2, step, 0)

    def conv_pair(layer, first, dst, residual, sums):
        shift = bias[layer]
        zero_tile = jnp.zeros((chans, chans), BF16)

        def tap(index):
            return zero_tile if index is None else wts[layer, index[0], index[1], index[2]]

        def block_pair(row):
            for kind, pieces in enumerate(PLAN):
                rhs = jnp.concatenate([jnp.concatenate([tap(t) for t in piece[2]], axis=1) for piece in pieces], axis=0)
                lhs = jnp.concatenate([act[first + f, pl.ds(row + di, ROWS)].reshape(ROWS * width, chans) for f, di, _ in pieces], axis=1)
                value = jnp.dot(lhs, rhs, preferred_element_type=F32).reshape(ROWS, width, 2 * chans)
                lo, hi = value[:, :, :chans], value[:, :, chans:]
                if kind < 2:
                    left_sum[:, kind, pl.ds(8, width), :] = lo
                    mid_sum[:, kind] = hi
                else:
                    right_sum[:, 0, pl.ds(8, width), :] = lo
                    right_sum[:, 1, pl.ds(8, width), :] = hi

        def finish(row, sums):
            for r in range(ROWS):
                for o in range(2):
                    value = mid_sum[r, o] + left_sum[r, o, pl.ds(7, width), :] + right_sum[r, o, pl.ds(9, width), :]
                    value = (value + shift).astype(BF16).astype(F32)
                    at = row + r
                    if residual:
                        value = (cur[first + o, at].astype(F32) + value).astype(BF16).astype(F32)
                    dst[first + o, at] = value.astype(BF16)
                    s1, s2 = row_sums(value)
                    sums = (sums[0] + s1, sums[1] + s2)
            return sums

        def step(i, sums):
            for u in range(UNROLL):
                row = (i * UNROLL + u) * ROWS
                block_pair(row)
                sums = finish(row, sums)
            return sums

        return lax.fori_loop(0, height // (ROWS * UNROLL), step, sums)

    def layer_step(block, odd, sums):
        layer = 2 * block + odd
        src, dst = (mid, cur) if odd else (cur, mid)
        norm_coefs(layer, sums)
        act_frames(src, range(n_frames), 2)
        sums = conv_pair(layer, 2, dst, odd == 1, zero_sums)

        def send_next():
            @pl.when(me < n_dev - 1)
            def _():
                halo_copy(dst, 1 - odd).start()

        if odd:

            @pl.when(block == 0)
            def _():
                send_next()

            @pl.when(block == 1)
            def _():
                pltpu.make_async_copy(cur.at[pl.ds(2, 2)], out.at[pl.ds(2, 2)], out_sem.at[1]).start()
        else:
            send_next()

        @pl.when(me == 0)
        def _():
            for f in range(2):
                def step(i, carry):
                    act[f, i + 1] = act[2, i + 1]
                    return carry

                lax.fori_loop(0, height, step, 0)

        @pl.when(me > 0)
        def _():
            halo_copy(src, odd).wait_recv()
            act_frames(halo.at[odd], range(2), 0)

        @pl.when(me < n_dev - 1)
        def _():
            halo_copy(src, odd).wait_send()

        return conv_pair(layer, 0, dst, odd == 1, sums)

    sums = zero_sums
    for f in range(n_frames):
        frame_loads[f].wait()
        sums = latent_sums(f, sums)
    for copy in wts_loads:
        copy.wait()

    def block_step(block, sums):
        return layer_step(block, 1, layer_step(block, 0, sums))

    lax.fori_loop(0, LAYERS // 2, block_step, sums)
    pltpu.make_async_copy(cur.at[pl.ds(0, 2)], out.at[pl.ds(0, 2)], out_sem.at[0]).start()
    pltpu.make_async_copy(cur.at[pl.ds(2, 2)], out.at[pl.ds(2, 2)], out_sem.at[1]).wait()
    pltpu.make_async_copy(cur.at[pl.ds(0, 2)], out.at[pl.ds(0, 2)], out_sem.at[0]).wait()


def solution(mesh):
    n_dev = mesh.shape["cp"]
    frame_spec = P(("dp", "cp"))

    def local_fn(latent, conv_kernels, conv_biases, gn_gammas, gn_betas):
        n_frames, height, width, chans = latent.shape
        far = n_dev // NEAR
        row = (LAYERS, 1, chans)
        vmem = pl.BlockSpec(memory_space=pltpu.VMEM)
        anywhere = pl.BlockSpec(memory_space=pl.ANY)
        dma = pltpu.SemaphoreType.DMA
        return pl.pallas_call(
            functools.partial(kernel, n_dev),
            out_shape=jax.ShapeDtypeStruct(latent.shape, BF16),
            in_specs=[anywhere, anywhere, vmem, vmem, vmem],
            out_specs=anywhere,
            scratch_shapes=[
                pltpu.VMEM(latent.shape, BF16),
                pltpu.VMEM(latent.shape, BF16),
                pltpu.VMEM((n_frames + 2, height + 2, width, chans), BF16),
                pltpu.VMEM((2, 2, height, width, chans), BF16),
                pltpu.VMEM(conv_kernels.shape, BF16),
                pltpu.VMEM((2, chans), F32),
                pltpu.VMEM((2, chans), F32),
                pltpu.VMEM((LAYERS, NEAR, 2, chans), F32),
                pltpu.VMEM((LAYERS, far, 2, chans), F32),
                pltpu.VMEM((2, 1, chans), F32),
                pltpu.VMEM((ROWS, 2, width, chans), F32),
                pltpu.VMEM((ROWS, 2, width + 16, chans), F32),
                pltpu.VMEM((ROWS, 2, width + 16, chans), F32),
                dma((n_frames,)),
                dma((LAYERS,)),
                dma((2,)),
                dma((2,)),
                dma((2,)),
                dma((NEAR,)),
                dma((LAYERS, NEAR)),
                dma((far,)),
                dma((LAYERS, far)),
            ],
            compiler_params=pltpu.CompilerParams(collective_id=0, has_side_effects=True, vmem_limit_bytes=60 * 1024 * 1024),
            name="resblocks",
        )(latent, conv_kernels, conv_biases.reshape(row), gn_gammas.reshape(row), gn_betas.reshape(row))

    return jax.shard_map(local_fn, mesh=mesh, in_specs=(frame_spec, P(), P(), P(), P()), out_specs=frame_spec, check_vma=False)
```

```python
import functools

import jax
import jax.numpy as jnp
from jax import lax
from jax.experimental import pallas as pl
from jax.experimental.pallas import tpu as pltpu
from jax.sharding import PartitionSpec as P

GROUP_WIDTH = 4
NORM_EPS = 1e-6
LAYERS = 4
LINE = 4
NEAR = 2 * LINE
ROWS = 6
UNROLL = 2
MESH = pl.DeviceIdType.MESH
BF16 = jnp.bfloat16
F32 = jnp.float32


def _plan():
    plan = []
    for out in range(2):
        pieces = [(out + k, di, ((k, di, 0), (k, di, 1))) for di in range(3) for k in range(3)]
        plan.append(pieces)
    pieces = []
    for di in range(3):
        for f in range(4):
            pieces.append((f, di, ((f, di, 2) if f < 3 else None, (f - 1, di, 2) if f > 0 else None)))
    plan.append(pieces)
    return plan


PLAN = _plan()


def kernel(n_dev, *refs):
    (lat, kern, bias, gamma, beta, out, cur, mid, act, halo, wts, part0, part1, part2, gat0, gat1, gat2, coef, mid_sum, left_sum, right_sum, load_sem, wts_sem, out_sem, halo_send, halo_recv, send0, recv0, send1, recv1, send2, recv2) = refs
    n_frames, height, width, chans = lat.shape
    far = n_dev // NEAR
    elem_count = float(n_dev * n_frames * height * width * GROUP_WIDTH)
    me = lax.axis_index("cp")
    near_pos = lax.rem(me, NEAR)
    far_pos = me // NEAR
    near_base = me - near_pos
    core = lax.rem(me, 2)
    line_pos = near_pos // 2
    partner = me + 1 - 2 * core

    def far_peer(j):
        slot = lax.rem(far_pos + j, far)
        return slot, slot * NEAR + near_pos

    barrier = pltpu.get_barrier_semaphore()
    for j in range(1, NEAR):
        pl.semaphore_signal(barrier, inc=1, device_id={"cp": near_base + lax.rem(near_pos + j, NEAR)}, device_id_type=MESH)
    for j in range(1, far):
        pl.semaphore_signal(barrier, inc=1, device_id={"cp": far_peer(j)[1]}, device_id_type=MESH)

    for device in (lax.rem(me + 1, n_dev), lax.rem(me + n_dev - 1, n_dev)):
        pl.semaphore_signal(barrier, inc=1, device_id={"cp": device}, device_id_type=MESH)

    frame_loads = [pltpu.make_async_copy(lat.at[f], cur.at[f], load_sem.at[f]) for f in range(n_frames)]
    for copy in frame_loads:
        copy.start()
    wts_loads = [pltpu.make_async_copy(kern.at[n], wts.at[n], wts_sem.at[n]) for n in range(LAYERS)]
    for copy in wts_loads:
        copy.start()

    pl.semaphore_wait(barrier, NEAR - 1 + far - 1 + 2)

    def halo_copy(src, slot):
        return pltpu.make_async_remote_copy(src_ref=src.at[pl.ds(n_frames - 2, 2)], dst_ref=halo.at[slot], send_sem=halo_send.at[slot], recv_sem=halo_recv.at[slot], device_id={"cp": me + 1}, device_id_type=MESH)

    @pl.when(me < n_dev - 1)
    def _():
        halo_copy(lat, 0).start()

    zero_row = jnp.zeros((width, chans), BF16)
    for f in range(n_frames + 2):
        act[f, 0] = zero_row
        act[f, height + 1] = zero_row
    edge = jnp.zeros((8, chans), F32)
    for r in range(ROWS):
        for o in range(2):
            left_sum[r, o, pl.ds(0, 8), :] = edge
            right_sum[r, o, pl.ds(width + 8, 8), :] = edge

    def row_sums(value):
        parts = value.reshape(width // 8, 8, chans)
        return jnp.sum(parts, axis=0), jnp.sum(parts * parts, axis=0)

    zero_sums = (jnp.zeros((8, chans), F32), jnp.zeros((8, chans), F32))

    def latent_sums(f, sums):
        def step(i, sums):
            for r in range(2):
                s1, s2 = row_sums(cur[f, 2 * i + r].astype(F32))
                sums = (sums[0] + s1, sums[1] + s2)
            return sums

        return lax.fori_loop(0, height // 2, step, sums)

    def group_total(sums):
        lane = lax.broadcasted_iota(jnp.int32, sums.shape, 1)
        for d in (1, 2):
            other = jnp.where(lax.rem(lane, 2 * d) < d, pltpu.roll(sums, chans - d, axis=1), pltpu.roll(sums, d, axis=1))
            sums = sums + other
        return sums

    def remote(src, dst, send, recv, device):
        return pltpu.make_async_remote_copy(src_ref=src, dst_ref=dst, send_sem=send, recv_sem=recv, device_id={"cp": device}, device_id_type=MESH)

    def in_order(gat, layer, size):
        total = gat[layer, 0]
        for slot in range(1, size):
            total = total + gat[layer, slot]
        return total

    def chip_sum(layer):
        copy = remote(part0, gat0.at[layer], send0, recv0.at[layer], partner)
        copy.start()
        copy.wait()
        return part0[...] + gat0[layer]

    def line_sum(layer):
        def copies():
            for j in range(1, LINE):
                slot = lax.rem(line_pos + j, LINE)
                for c in range(2):
                    yield remote(part1, gat1.at[layer, line_pos], send1.at[j, c], recv1.at[layer, line_pos], near_base + 2 * slot + c)

        @pl.when(core == 0)
        def _():
            for copy in copies():
                copy.start()

        gat1[layer, line_pos] = part1[...]
        for j in range(1, LINE):
            slot = lax.rem(line_pos + j, LINE)
            remote(part1, gat1.at[layer, slot], send1.at[j, 0], recv1.at[layer, slot], me).wait_recv()
        total = in_order(gat1, layer, LINE)

        @pl.when(core == 0)
        def _():
            for copy in copies():
                copy.wait_send()

        return total

    def far_sum(layer):
        for j in range(1, far):
            remote(part2, gat2.at[layer, far_pos], send2.at[j], recv2.at[layer, far_pos], far_peer(j)[1]).start()
        gat2[layer, far_pos] = part2[...]
        for j in range(1, far):
            slot, device = far_peer(j)
            remote(part2, gat2.at[layer, slot], send2.at[j], recv2.at[layer, slot], device).wait_recv()
        total = in_order(gat2, layer, far)
        for j in range(1, far):
            remote(part2, gat2.at[layer, far_pos], send2.at[j], recv2.at[layer, far_pos], far_peer(j)[1]).wait_send()
        return total

    def norm_coefs(layer, sums):
        part0[...] = jnp.concatenate([jnp.sum(sums[0], axis=0, keepdims=True), jnp.sum(sums[1], axis=0, keepdims=True)], axis=0)
        part1[...] = chip_sum(layer)
        part2[...] = line_sum(layer)
        total = far_sum(layer)
        total = group_total(total)
        mean = total[0:1] / elem_count
        var = total[1:2] / elem_count - mean * mean
        scale = lax.rsqrt(var + NORM_EPS) * gamma[layer]
        coef[0] = scale
        coef[1] = beta[layer] - mean * scale

    def act_rows(value):
        normed = (value.astype(F32) * coef[0] + coef[1]).astype(BF16).astype(F32)
        half = normed * 0.5
        return (half + half * jnp.tanh(half)).astype(BF16)

    def act_frames(src, frames, first):
        def step(i, carry):
            for f in frames:
                for r in range(2):
                    act[first + f, 2 * i + r + 1] = act_rows(src[f, 2 * i + r])
            return carry

        lax.fori_loop(0, height // 2, step, 0)

    def conv_pair(layer, first, dst, residual, sums):
        shift = bias[layer]
        zero_tile = jnp.zeros((chans, chans), BF16)

        def tap(index):
            return zero_tile if index is None else wts[layer, index[0], index[1], index[2]]

        def block_pair(row):
            for kind, pieces in enumerate(PLAN):
                rhs = jnp.concatenate([jnp.concatenate([tap(t) for t in piece[2]], axis=1) for piece in pieces], axis=0)
                lhs = jnp.concatenate([act[first + f, pl.ds(row + di, ROWS)].reshape(ROWS * width, chans) for f, di, _ in pieces], axis=1)
                value = jnp.dot(lhs, rhs, preferred_element_type=F32).reshape(ROWS, width, 2 * chans)
                lo, hi = value[:, :, :chans], value[:, :, chans:]
                if kind < 2:
                    left_sum[:, kind, pl.ds(8, width), :] = lo
                    mid_sum[:, kind] = hi
                else:
                    right_sum[:, 0, pl.ds(8, width), :] = lo
                    right_sum[:, 1, pl.ds(8, width), :] = hi

        def finish(row, sums):
            for r in range(ROWS):
                for o in range(2):
                    value = mid_sum[r, o] + left_sum[r, o, pl.ds(7, width), :] + right_sum[r, o, pl.ds(9, width), :]
                    value = (value + shift).astype(BF16).astype(F32)
                    at = row + r
                    if residual:
                        value = (cur[first + o, at].astype(F32) + value).astype(BF16).astype(F32)
                    dst[first + o, at] = value.astype(BF16)
                    s1, s2 = row_sums(value)
                    sums = (sums[0] + s1, sums[1] + s2)
            return sums

        def step(i, sums):
            for u in range(UNROLL):
                row = (i * UNROLL + u) * ROWS
                block_pair(row)
                sums = finish(row, sums)
            return sums

        return lax.fori_loop(0, height // (ROWS * UNROLL), step, sums)

    def layer_step(block, odd, sums):
        layer = 2 * block + odd
        src, dst = (mid, cur) if odd else (cur, mid)
        norm_coefs(layer, sums)
        act_frames(src, range(n_frames), 2)
        sums = conv_pair(layer, 2, dst, odd == 1, zero_sums)

        def send_next():
            @pl.when(me < n_dev - 1)
            def _():
                halo_copy(dst, 1 - odd).start()

        if odd:

            @pl.when(block == 0)
            def _():
                send_next()

            @pl.when(block == 1)
            def _():
                pltpu.make_async_copy(cur.at[pl.ds(2, 2)], out.at[pl.ds(2, 2)], out_sem.at[1]).start()
        else:
            send_next()

        @pl.when(me == 0)
        def _():
            for f in range(2):
                def step(i, carry):
                    act[f, i + 1] = act[2, i + 1]
                    return carry

                lax.fori_loop(0, height, step, 0)

        @pl.when(me > 0)
        def _():
            halo_copy(src, odd).wait_recv()
            act_frames(halo.at[odd], range(2), 0)

        @pl.when(me < n_dev - 1)
        def _():
            halo_copy(src, odd).wait_send()

        return conv_pair(layer, 0, dst, odd == 1, sums)

    sums = zero_sums
    for f in range(n_frames):
        frame_loads[f].wait()
        sums = latent_sums(f, sums)
    for copy in wts_loads:
        copy.wait()

    def block_step(block, sums):
        return layer_step(block, 1, layer_step(block, 0, sums))

    lax.fori_loop(0, LAYERS // 2, block_step, sums)
    pltpu.make_async_copy(cur.at[pl.ds(0, 2)], out.at[pl.ds(0, 2)], out_sem.at[0]).start()
    pltpu.make_async_copy(cur.at[pl.ds(2, 2)], out.at[pl.ds(2, 2)], out_sem.at[1]).wait()
    pltpu.make_async_copy(cur.at[pl.ds(0, 2)], out.at[pl.ds(0, 2)], out_sem.at[0]).wait()


def solution(mesh):
    n_dev = mesh.shape["cp"]
    frame_spec = P(("dp", "cp"))

    def local_fn(latent, conv_kernels, conv_biases, gn_gammas, gn_betas):
        n_frames, height, width, chans = latent.shape
        far = n_dev // NEAR
        row = (LAYERS, 1, chans)
        vmem = pl.BlockSpec(memory_space=pltpu.VMEM)
        anywhere = pl.BlockSpec(memory_space=pl.ANY)
        dma = pltpu.SemaphoreType.DMA
        return pl.pallas_call(
            functools.partial(kernel, n_dev),
            out_shape=jax.ShapeDtypeStruct(latent.shape, BF16),
            in_specs=[anywhere, anywhere, vmem, vmem, vmem],
            out_specs=anywhere,
            scratch_shapes=[
                pltpu.VMEM(latent.shape, BF16),
                pltpu.VMEM(latent.shape, BF16),
                pltpu.VMEM((n_frames + 2, height + 2, width, chans), BF16),
                pltpu.VMEM((2, 2, height, width, chans), BF16),
                pltpu.VMEM(conv_kernels.shape, BF16),
                pltpu.VMEM((2, chans), F32),
                pltpu.VMEM((2, chans), F32),
                pltpu.VMEM((2, chans), F32),
                pltpu.VMEM((LAYERS, 2, chans), F32),
                pltpu.VMEM((LAYERS, LINE, 2, chans), F32),
                pltpu.VMEM((LAYERS, far, 2, chans), F32),
                pltpu.VMEM((2, 1, chans), F32),
                pltpu.VMEM((ROWS, 2, width, chans), F32),
                pltpu.VMEM((ROWS, 2, width + 16, chans), F32),
                pltpu.VMEM((ROWS, 2, width + 16, chans), F32),
                dma((n_frames,)),
                dma((LAYERS,)),
                dma((2,)),
                dma((2,)),
                dma((2,)),
                dma,
                dma((LAYERS,)),
                dma((LINE, 2)),
                dma((LAYERS, LINE)),
                dma((far,)),
                dma((LAYERS, far)),
            ],
            compiler_params=pltpu.CompilerParams(collective_id=0, has_side_effects=True, vmem_limit_bytes=60 * 1024 * 1024),
            name="resblocks",
        )(latent, conv_kernels, conv_biases.reshape(row), gn_gammas.reshape(row), gn_betas.reshape(row))

    return jax.shard_map(local_fn, mesh=mesh, in_specs=(frame_spec, P(), P(), P(), P()), out_specs=frame_spec, check_vma=False)
```

```python
import functools

import jax
import jax.numpy as jnp
from jax import lax
from jax.experimental import pallas as pl
from jax.experimental.pallas import tpu as pltpu
from jax.sharding import PartitionSpec as P

GROUP_WIDTH = 4
NORM_EPS = 1e-6
LAYERS = 4
LINE = 4
NEAR = 2 * LINE
CHUNK = 6
EARLY = 3
ROWS = 6
UNROLL = 2
STEP_ROWS = ROWS * UNROLL
MESH = pl.DeviceIdType.MESH
BF16 = jnp.bfloat16
F32 = jnp.float32


def _plan():
    plan = []
    for out in range(2):
        pieces = [(out + k, di, ((k, di, 0), (k, di, 1))) for di in range(3) for k in range(3)]
        plan.append(pieces)
    pieces = []
    for di in range(3):
        for f in range(4):
            pieces.append((f, di, ((f, di, 2) if f < 3 else None, (f - 1, di, 2) if f > 0 else None)))
    plan.append(pieces)
    return plan


PLAN = _plan()


def kernel(n_dev, *refs):
    (lat, kern, bias, gamma, beta, out, cur, mid, act, halo, wts, part0, part1, part2, gat0, gat1, gat2, coef, mid_sum, left_sum, right_sum, load_sem, wts_sem, out_sem, halo_send, halo_recv, send0, recv0, send1, recv1, send2, recv2) = refs
    n_frames, height, width, chans = lat.shape
    far = n_dev // NEAR
    elem_count = float(n_dev * n_frames * height * width * GROUP_WIDTH)
    me = lax.axis_index("cp")
    near_pos = lax.rem(me, NEAR)
    far_pos = me // NEAR
    near_base = me - near_pos
    core = lax.rem(me, 2)
    line_pos = near_pos // 2
    partner = me + 1 - 2 * core

    def far_peer(j):
        slot = lax.rem(far_pos + j, far)
        return slot, slot * NEAR + near_pos

    barrier = pltpu.get_barrier_semaphore()
    for j in range(1, NEAR):
        pl.semaphore_signal(barrier, inc=1, device_id={"cp": near_base + lax.rem(near_pos + j, NEAR)}, device_id_type=MESH)
    for j in range(1, far):
        pl.semaphore_signal(barrier, inc=1, device_id={"cp": far_peer(j)[1]}, device_id_type=MESH)

    for device in (lax.rem(me + 1, n_dev), lax.rem(me + n_dev - 1, n_dev)):
        pl.semaphore_signal(barrier, inc=1, device_id={"cp": device}, device_id_type=MESH)

    frame_loads = [pltpu.make_async_copy(lat.at[f], cur.at[f], load_sem.at[f]) for f in range(n_frames)]
    for copy in frame_loads:
        copy.start()
    wts_loads = [pltpu.make_async_copy(kern.at[n], wts.at[n], wts_sem.at[n]) for n in range(LAYERS)]
    for copy in wts_loads:
        copy.start()

    pl.semaphore_wait(barrier, NEAR - 1 + far - 1 + 2)

    n_chunks = height // CHUNK

    def halo_copy(src, slot, chunk):
        rows = pl.ds(chunk * CHUNK, CHUNK)
        return pltpu.make_async_remote_copy(src_ref=src.at[pl.ds(n_frames - 2, 2), rows], dst_ref=halo.at[slot, :, rows], send_sem=halo_send.at[slot, chunk], recv_sem=halo_recv.at[slot, chunk], device_id={"cp": me + 1}, device_id_type=MESH)

    def send_halo(src, slot, chunks):
        @pl.when(me < n_dev - 1)
        def _():
            for chunk in chunks:
                halo_copy(src, slot, chunk).start()

    send_halo(lat, 0, range(EARLY))

    zero_row = jnp.zeros((width, chans), BF16)
    for f in range(n_frames + 2):
        act[f, 0] = zero_row
        act[f, height + 1] = zero_row
    edge = jnp.zeros((8, chans), F32)
    for r in range(ROWS):
        for o in range(2):
            left_sum[r, o, pl.ds(0, 8), :] = edge
            right_sum[r, o, pl.ds(width + 8, 8), :] = edge

    def row_sums(value):
        parts = value.reshape(width // 8, 8, chans)
        return jnp.sum(parts, axis=0), jnp.sum(parts * parts, axis=0)

    zero_sums = (jnp.zeros((8, chans), F32), jnp.zeros((8, chans), F32))

    def latent_sums(f, sums):
        def step(i, sums):
            for r in range(2):
                s1, s2 = row_sums(cur[f, 2 * i + r].astype(F32))
                sums = (sums[0] + s1, sums[1] + s2)
            return sums

        return lax.fori_loop(0, height // 2, step, sums)

    def group_total(sums):
        lane = lax.broadcasted_iota(jnp.int32, sums.shape, 1)
        for d in (1, 2):
            other = jnp.where(lax.rem(lane, 2 * d) < d, pltpu.roll(sums, chans - d, axis=1), pltpu.roll(sums, d, axis=1))
            sums = sums + other
        return sums

    def remote(src, dst, send, recv, device):
        return pltpu.make_async_remote_copy(src_ref=src, dst_ref=dst, send_sem=send, recv_sem=recv, device_id={"cp": device}, device_id_type=MESH)

    def in_order(gat, layer, size):
        total = gat[layer, 0]
        for slot in range(1, size):
            total = total + gat[layer, slot]
        return total

    def chip_sum(layer):
        copy = remote(part0, gat0.at[layer], send0, recv0.at[layer], partner)
        copy.start()
        copy.wait()
        return part0[...] + gat0[layer]

    def line_sum(layer):
        def copies():
            for j in range(1, LINE):
                slot = lax.rem(line_pos + j, LINE)
                for c in range(2):
                    yield remote(part1, gat1.at[layer, line_pos], send1.at[j, c], recv1.at[layer, line_pos], near_base + 2 * slot + c)

        @pl.when(core == 0)
        def _():
            for copy in copies():
                copy.start()

        gat1[layer, line_pos] = part1[...]
        for j in range(1, LINE):
            slot = lax.rem(line_pos + j, LINE)
            remote(part1, gat1.at[layer, slot], send1.at[j, 0], recv1.at[layer, slot], me).wait_recv()
        total = in_order(gat1, layer, LINE)

        @pl.when(core == 0)
        def _():
            for copy in copies():
                copy.wait_send()

        return total

    def far_sum(layer):
        for j in range(1, far):
            remote(part2, gat2.at[layer, far_pos], send2.at[j], recv2.at[layer, far_pos], far_peer(j)[1]).start()
        gat2[layer, far_pos] = part2[...]
        for j in range(1, far):
            slot, device = far_peer(j)
            remote(part2, gat2.at[layer, slot], send2.at[j], recv2.at[layer, slot], device).wait_recv()
        total = in_order(gat2, layer, far)
        for j in range(1, far):
            remote(part2, gat2.at[layer, far_pos], send2.at[j], recv2.at[layer, far_pos], far_peer(j)[1]).wait_send()
        return total

    def norm_coefs(layer, sums):
        part0[...] = jnp.concatenate([jnp.sum(sums[0], axis=0, keepdims=True), jnp.sum(sums[1], axis=0, keepdims=True)], axis=0)
        part1[...] = chip_sum(layer)
        part2[...] = line_sum(layer)
        total = far_sum(layer)
        total = group_total(total)
        mean = total[0:1] / elem_count
        var = total[1:2] / elem_count - mean * mean
        scale = lax.rsqrt(var + NORM_EPS) * gamma[layer]
        coef[0] = scale
        coef[1] = beta[layer] - mean * scale

    def act_rows(value):
        normed = (value.astype(F32) * coef[0] + coef[1]).astype(BF16).astype(F32)
        half = normed * 0.5
        return (half + half * jnp.tanh(half)).astype(BF16)

    def act_frames(src, frames, first, start=0, rows=height):
        def step(i, carry):
            for f in frames:
                for r in range(2):
                    at = start + 2 * i + r
                    act[first + f, at + 1] = act_rows(src[f, at])
            return carry

        lax.fori_loop(0, rows // 2, step, 0)

    def conv_pair(layer, first, dst, residual, sums, before=None):
        shift = bias[layer]
        zero_tile = jnp.zeros((chans, chans), BF16)

        def tap(index):
            return zero_tile if index is None else wts[layer, index[0], index[1], index[2]]

        def block_pair(row):
            for kind, pieces in enumerate(PLAN):
                rhs = jnp.concatenate([jnp.concatenate([tap(t) for t in piece[2]], axis=1) for piece in pieces], axis=0)
                lhs = jnp.concatenate([act[first + f, pl.ds(row + di, ROWS)].reshape(ROWS * width, chans) for f, di, _ in pieces], axis=1)
                value = jnp.dot(lhs, rhs, preferred_element_type=F32).reshape(ROWS, width, 2 * chans)
                lo, hi = value[:, :, :chans], value[:, :, chans:]
                if kind < 2:
                    left_sum[:, kind, pl.ds(8, width), :] = lo
                    mid_sum[:, kind] = hi
                else:
                    right_sum[:, 0, pl.ds(8, width), :] = lo
                    right_sum[:, 1, pl.ds(8, width), :] = hi

        def finish(row, sums):
            for r in range(ROWS):
                for o in range(2):
                    value = mid_sum[r, o] + left_sum[r, o, pl.ds(7, width), :] + right_sum[r, o, pl.ds(9, width), :]
                    value = (value + shift).astype(BF16).astype(F32)
                    at = row + r
                    if residual:
                        value = (cur[first + o, at].astype(F32) + value).astype(BF16).astype(F32)
                    dst[first + o, at] = value.astype(BF16)
                    s1, s2 = row_sums(value)
                    sums = (sums[0] + s1, sums[1] + s2)
            return sums

        def step(i, sums):
            if before is not None:
                before(i)
            for u in range(UNROLL):
                row = (i * UNROLL + u) * ROWS
                block_pair(row)
                sums = finish(row, sums)
            return sums

        return lax.fori_loop(0, height // (ROWS * UNROLL), step, sums)

    def layer_step(block, odd, sums):
        layer = 2 * block + odd
        src, dst = (mid, cur) if odd else (cur, mid)
        norm_coefs(layer, sums)
        in_step = STEP_ROWS // CHUNK
        late = n_chunks - in_step

        if odd:
            send_halo(src, odd, range(late, n_chunks))
        else:

            @pl.when(block == 0)
            def _():
                send_halo(lat, odd, range(EARLY, n_chunks))

            @pl.when(block > 0)
            def _():
                send_halo(src, odd, range(late, n_chunks))

        act_frames(src, range(n_frames), 2)

        def send_done_rows(i):
            @pl.when((me < n_dev - 1) & (layer < LAYERS - 1) & (i > 0))
            def _():
                for c in range(in_step):
                    halo_copy(dst, 1 - odd, (i - 1) * in_step + c).start()

        sums = conv_pair(layer, 2, dst, odd == 1, zero_sums, send_done_rows)
        if odd:

            @pl.when(block == 1)
            def _():
                pltpu.make_async_copy(cur.at[pl.ds(2, 2)], out.at[pl.ds(2, 2)], out_sem.at[1]).start()

        def take_chunk(chunk):
            halo_copy(src, odd, chunk).wait_recv()
            act_frames(halo.at[odd], range(2), 0, chunk * CHUNK, CHUNK)

        def take_rows(i):
            for c in range(in_step):
                chunk = i * in_step + c + 1

                @pl.when((me > 0) & (chunk < n_chunks))
                def _():
                    take_chunk(chunk)

        @pl.when(me == 0)
        def _():
            for f in range(2):
                def step(i, carry):
                    act[f, i + 1] = act[2, i + 1]
                    return carry

                lax.fori_loop(0, height, step, 0)

        @pl.when(me > 0)
        def _():
            take_chunk(0)

        sums = conv_pair(layer, 0, dst, odd == 1, sums, take_rows)

        @pl.when(me < n_dev - 1)
        def _():
            for chunk in range(n_chunks):
                halo_copy(src, odd, chunk).wait_send()

        return sums

    sums = zero_sums
    for f in range(n_frames):
        frame_loads[f].wait()
        sums = latent_sums(f, sums)
    for copy in wts_loads:
        copy.wait()

    def block_step(block, sums):
        return layer_step(block, 1, layer_step(block, 0, sums))

    lax.fori_loop(0, LAYERS // 2, block_step, sums)
    pltpu.make_async_copy(cur.at[pl.ds(0, 2)], out.at[pl.ds(0, 2)], out_sem.at[0]).start()
    pltpu.make_async_copy(cur.at[pl.ds(2, 2)], out.at[pl.ds(2, 2)], out_sem.at[1]).wait()
    pltpu.make_async_copy(cur.at[pl.ds(0, 2)], out.at[pl.ds(0, 2)], out_sem.at[0]).wait()


def solution(mesh):
    n_dev = mesh.shape["cp"]
    frame_spec = P(("dp", "cp"))

    def local_fn(latent, conv_kernels, conv_biases, gn_gammas, gn_betas):
        n_frames, height, width, chans = latent.shape
        far = n_dev // NEAR
        row = (LAYERS, 1, chans)
        vmem = pl.BlockSpec(memory_space=pltpu.VMEM)
        anywhere = pl.BlockSpec(memory_space=pl.ANY)
        dma = pltpu.SemaphoreType.DMA
        return pl.pallas_call(
            functools.partial(kernel, n_dev),
            out_shape=jax.ShapeDtypeStruct(latent.shape, BF16),
            in_specs=[anywhere, anywhere, vmem, vmem, vmem],
            out_specs=anywhere,
            scratch_shapes=[
                pltpu.VMEM(latent.shape, BF16),
                pltpu.VMEM(latent.shape, BF16),
                pltpu.VMEM((n_frames + 2, height + 2, width, chans), BF16),
                pltpu.VMEM((2, 2, height, width, chans), BF16),
                pltpu.VMEM(conv_kernels.shape, BF16),
                pltpu.VMEM((2, chans), F32),
                pltpu.VMEM((2, chans), F32),
                pltpu.VMEM((2, chans), F32),
                pltpu.VMEM((LAYERS, 2, chans), F32),
                pltpu.VMEM((LAYERS, LINE, 2, chans), F32),
                pltpu.VMEM((LAYERS, far, 2, chans), F32),
                pltpu.VMEM((2, 1, chans), F32),
                pltpu.VMEM((ROWS, 2, width, chans), F32),
                pltpu.VMEM((ROWS, 2, width + 16, chans), F32),
                pltpu.VMEM((ROWS, 2, width + 16, chans), F32),
                dma((n_frames,)),
                dma((LAYERS,)),
                dma((2,)),
                dma((2, height // CHUNK)),
                dma((2, height // CHUNK)),
                dma,
                dma((LAYERS,)),
                dma((LINE, 2)),
                dma((LAYERS, LINE)),
                dma((far,)),
                dma((LAYERS, far)),
            ],
            compiler_params=pltpu.CompilerParams(collective_id=0, has_side_effects=True, vmem_limit_bytes=60 * 1024 * 1024),
            name="resblocks",
        )(latent, conv_kernels, conv_biases.reshape(row), gn_gammas.reshape(row), gn_betas.reshape(row))

    return jax.shard_map(local_fn, mesh=mesh, in_specs=(frame_spec, P(), P(), P(), P()), out_specs=frame_spec, check_vma=False)
```

```python
import functools

import jax
import jax.numpy as jnp
from jax import lax
from jax.experimental import pallas as pl
from jax.experimental.pallas import tpu as pltpu
from jax.sharding import PartitionSpec as P

GROUP_WIDTH = 4
NORM_EPS = 1e-6
LAYERS = 4
LINE = 4
NEAR = 2 * LINE
CHUNK = 6
EARLY = 3
ROWS = 6
UNROLL = 2
STEP_ROWS = ROWS * UNROLL
MESH = pl.DeviceIdType.MESH
BF16 = jnp.bfloat16
F32 = jnp.float32


def _plan():
    plan = []
    for out in range(2):
        pieces = [(out + k, di, ((k, di, 0), (k, di, 1))) for di in range(3) for k in range(3)]
        plan.append(pieces)
    pieces = []
    for di in range(3):
        for f in range(4):
            pieces.append((f, di, ((f, di, 2) if f < 3 else None, (f - 1, di, 2) if f > 0 else None)))
    plan.append(pieces)
    return plan


PLAN = _plan()


def kernel(n_dev, *refs):
    (lat, kern, bias, gamma, beta, out, cur, mid, act, halo, wts, part0, part1, part2, gat0, gat1, gat2, coef, mid_sum, left_sum, right_sum, load_sem, wts_sem, out_sem, halo_send, halo_recv, send0, recv0, send1, recv1, send2, recv2) = refs
    n_frames, height, width, chans = lat.shape
    far = n_dev // NEAR
    elem_count = float(n_dev * n_frames * height * width * GROUP_WIDTH)
    me = lax.axis_index("cp")
    near_pos = lax.rem(me, NEAR)
    far_pos = me // NEAR
    near_base = me - near_pos
    core = lax.rem(me, 2)
    line_pos = near_pos // 2
    partner = me + 1 - 2 * core

    def far_peer(j):
        slot = lax.rem(far_pos + j, far)
        return slot, slot * NEAR + near_pos

    frame_loads = [pltpu.make_async_copy(lat.at[f], cur.at[f], load_sem.at[f]) for f in range(n_frames)]
    for copy in frame_loads:
        copy.start()
    wts_loads = [pltpu.make_async_copy(kern.at[n], wts.at[n], wts_sem.at[n]) for n in range(LAYERS)]
    for copy in wts_loads:
        copy.start()

    n_chunks = height // CHUNK

    def halo_copy(src, slot, chunk):
        rows = pl.ds(chunk * CHUNK, CHUNK)
        return pltpu.make_async_remote_copy(src_ref=src.at[pl.ds(n_frames - 2, 2), rows], dst_ref=halo.at[slot, :, rows], send_sem=halo_send.at[slot, chunk], recv_sem=halo_recv.at[slot, chunk], device_id={"cp": me + 1}, device_id_type=MESH)

    def send_halo(src, slot, chunks):
        @pl.when(me < n_dev - 1)
        def _():
            for chunk in chunks:
                halo_copy(src, slot, chunk).start()

    send_halo(lat, 0, range(EARLY))

    zero_row = jnp.zeros((width, chans), BF16)
    for f in range(n_frames + 2):
        act[f, 0] = zero_row
        act[f, height + 1] = zero_row
    edge = jnp.zeros((8, chans), F32)
    for r in range(ROWS):
        for o in range(2):
            left_sum[r, o, pl.ds(0, 8), :] = edge
            right_sum[r, o, pl.ds(width + 8, 8), :] = edge

    def row_sums(value):
        parts = value.reshape(width // 8, 8, chans)
        return jnp.sum(parts, axis=0), jnp.sum(parts * parts, axis=0)

    zero_sums = (jnp.zeros((8, chans), F32), jnp.zeros((8, chans), F32))

    def latent_sums(f, sums):
        def step(i, sums):
            for r in range(2):
                s1, s2 = row_sums(cur[f, 2 * i + r].astype(F32))
                sums = (sums[0] + s1, sums[1] + s2)
            return sums

        return lax.fori_loop(0, height // 2, step, sums)

    def group_total(sums):
        lane = lax.broadcasted_iota(jnp.int32, sums.shape, 1)
        for d in (1, 2):
            other = jnp.where(lax.rem(lane, 2 * d) < d, pltpu.roll(sums, chans - d, axis=1), pltpu.roll(sums, d, axis=1))
            sums = sums + other
        return sums

    def remote(src, dst, send, recv, device):
        return pltpu.make_async_remote_copy(src_ref=src, dst_ref=dst, send_sem=send, recv_sem=recv, device_id={"cp": device}, device_id_type=MESH)

    def in_order(gat, layer, size):
        total = gat[layer, 0]
        for slot in range(1, size):
            total = total + gat[layer, slot]
        return total

    def chip_sum(layer):
        copy = remote(part0, gat0.at[layer], send0, recv0.at[layer], partner)
        copy.start()
        copy.wait()
        return part0[...] + gat0[layer]

    def line_sum(layer):
        def copies():
            for j in range(1, LINE):
                slot = lax.rem(line_pos + j, LINE)
                for c in range(2):
                    yield remote(part1, gat1.at[layer, line_pos], send1.at[j, c], recv1.at[layer, line_pos], near_base + 2 * slot + c)

        @pl.when(core == 0)
        def _():
            for copy in copies():
                copy.start()

        gat1[layer, line_pos] = part1[...]
        for j in range(1, LINE):
            slot = lax.rem(line_pos + j, LINE)
            remote(part1, gat1.at[layer, slot], send1.at[j, 0], recv1.at[layer, slot], me).wait_recv()
        total = in_order(gat1, layer, LINE)

        @pl.when(core == 0)
        def _():
            for copy in copies():
                copy.wait_send()

        return total

    def far_sum(layer):
        for j in range(1, far):
            remote(part2, gat2.at[layer, far_pos], send2.at[j], recv2.at[layer, far_pos], far_peer(j)[1]).start()
        gat2[layer, far_pos] = part2[...]
        for j in range(1, far):
            slot, device = far_peer(j)
            remote(part2, gat2.at[layer, slot], send2.at[j], recv2.at[layer, slot], device).wait_recv()
        total = in_order(gat2, layer, far)
        for j in range(1, far):
            remote(part2, gat2.at[layer, far_pos], send2.at[j], recv2.at[layer, far_pos], far_peer(j)[1]).wait_send()
        return total

    def norm_coefs(layer, sums):
        part0[...] = jnp.concatenate([jnp.sum(sums[0], axis=0, keepdims=True), jnp.sum(sums[1], axis=0, keepdims=True)], axis=0)
        part1[...] = chip_sum(layer)
        part2[...] = line_sum(layer)
        total = far_sum(layer)
        total = group_total(total)
        mean = total[0:1] / elem_count
        var = total[1:2] / elem_count - mean * mean
        scale = lax.rsqrt(var + NORM_EPS) * gamma[layer]
        coef[0] = scale
        coef[1] = beta[layer] - mean * scale

    def act_rows(value):
        normed = (value.astype(F32) * coef[0] + coef[1]).astype(BF16).astype(F32)
        half = normed * 0.5
        return (half + half * jnp.tanh(half)).astype(BF16)

    def act_frames(src, frames, first, start=0, rows=height):
        def step(i, carry):
            for f in frames:
                for r in range(2):
                    at = start + 2 * i + r
                    act[first + f, at + 1] = act_rows(src[f, at])
            return carry

        lax.fori_loop(0, rows // 2, step, 0)

    def conv_pair(layer, first, dst, residual, sums, before=None):
        shift = bias[layer]
        zero_tile = jnp.zeros((chans, chans), BF16)

        def tap(index):
            return zero_tile if index is None else wts[layer, index[0], index[1], index[2]]

        def block_pair(row):
            for kind, pieces in enumerate(PLAN):
                rhs = jnp.concatenate([jnp.concatenate([tap(t) for t in piece[2]], axis=1) for piece in pieces], axis=0)
                lhs = jnp.concatenate([act[first + f, pl.ds(row + di, ROWS)].reshape(ROWS * width, chans) for f, di, _ in pieces], axis=1)
                value = jnp.dot(lhs, rhs, preferred_element_type=F32).reshape(ROWS, width, 2 * chans)
                lo, hi = value[:, :, :chans], value[:, :, chans:]
                if kind < 2:
                    left_sum[:, kind, pl.ds(8, width), :] = lo
                    mid_sum[:, kind] = hi
                else:
                    right_sum[:, 0, pl.ds(8, width), :] = lo
                    right_sum[:, 1, pl.ds(8, width), :] = hi

        def finish(row, sums):
            for r in range(ROWS):
                for o in range(2):
                    value = mid_sum[r, o] + left_sum[r, o, pl.ds(7, width), :] + right_sum[r, o, pl.ds(9, width), :]
                    value = (value + shift).astype(BF16).astype(F32)
                    at = row + r
                    if residual:
                        value = (cur[first + o, at].astype(F32) + value).astype(BF16).astype(F32)
                    dst[first + o, at] = value.astype(BF16)
                    s1, s2 = row_sums(value)
                    sums = (sums[0] + s1, sums[1] + s2)
            return sums

        def step(i, sums):
            if before is not None:
                before(i)
            for u in range(UNROLL):
                row = (i * UNROLL + u) * ROWS
                block_pair(row)
                sums = finish(row, sums)
            return sums

        return lax.fori_loop(0, height // (ROWS * UNROLL), step, sums)

    def layer_step(block, odd, sums):
        layer = 2 * block + odd
        src, dst = (mid, cur) if odd else (cur, mid)
        norm_coefs(layer, sums)
        in_step = STEP_ROWS // CHUNK
        late = n_chunks - in_step

        if odd:
            send_halo(src, odd, range(late, n_chunks))
        else:

            @pl.when(block == 0)
            def _():
                send_halo(lat, odd, range(EARLY, n_chunks))

            @pl.when(block > 0)
            def _():
                send_halo(src, odd, range(late, n_chunks))

        act_frames(src, range(n_frames), 2)

        def send_done_rows(i):
            @pl.when((me < n_dev - 1) & (layer < LAYERS - 1) & (i > 0))
            def _():
                for c in range(in_step):
                    halo_copy(dst, 1 - odd, (i - 1) * in_step + c).start()

        sums = conv_pair(layer, 2, dst, odd == 1, zero_sums, send_done_rows)
        if odd:

            @pl.when(block == 1)
            def _():
                pltpu.make_async_copy(cur.at[pl.ds(2, 2)], out.at[pl.ds(2, 2)], out_sem.at[1]).start()

        def take_chunk(chunk):
            halo_copy(src, odd, chunk).wait_recv()
            act_frames(halo.at[odd], range(2), 0, chunk * CHUNK, CHUNK)

        def take_rows(i):
            for c in range(in_step):
                chunk = i * in_step + c + 1

                @pl.when((me > 0) & (chunk < n_chunks))
                def _():
                    take_chunk(chunk)

        @pl.when(me == 0)
        def _():
            for f in range(2):
                def step(i, carry):
                    act[f, i + 1] = act[2, i + 1]
                    return carry

                lax.fori_loop(0, height, step, 0)

        @pl.when(me > 0)
        def _():
            take_chunk(0)

        sums = conv_pair(layer, 0, dst, odd == 1, sums, take_rows)

        @pl.when(me < n_dev - 1)
        def _():
            for chunk in range(n_chunks):
                halo_copy(src, odd, chunk).wait_send()

        return sums

    sums = zero_sums
    for f in range(n_frames):
        frame_loads[f].wait()
        sums = latent_sums(f, sums)
    for copy in wts_loads:
        copy.wait()

    def block_step(block, sums):
        return layer_step(block, 1, layer_step(block, 0, sums))

    lax.fori_loop(0, LAYERS // 2, block_step, sums)
    pltpu.make_async_copy(cur.at[pl.ds(0, 2)], out.at[pl.ds(0, 2)], out_sem.at[0]).start()
    pltpu.make_async_copy(cur.at[pl.ds(2, 2)], out.at[pl.ds(2, 2)], out_sem.at[1]).wait()
    pltpu.make_async_copy(cur.at[pl.ds(0, 2)], out.at[pl.ds(0, 2)], out_sem.at[0]).wait()


def solution(mesh):
    n_dev = mesh.shape["cp"]
    frame_spec = P(("dp", "cp"))

    def local_fn(latent, conv_kernels, conv_biases, gn_gammas, gn_betas):
        n_frames, height, width, chans = latent.shape
        far = n_dev // NEAR
        row = (LAYERS, 1, chans)
        vmem = pl.BlockSpec(memory_space=pltpu.VMEM)
        anywhere = pl.BlockSpec(memory_space=pl.ANY)
        dma = pltpu.SemaphoreType.DMA
        return pl.pallas_call(
            functools.partial(kernel, n_dev),
            out_shape=jax.ShapeDtypeStruct(latent.shape, BF16),
            in_specs=[anywhere, anywhere, vmem, vmem, vmem],
            out_specs=anywhere,
            scratch_shapes=[
                pltpu.VMEM(latent.shape, BF16),
                pltpu.VMEM(latent.shape, BF16),
                pltpu.VMEM((n_frames + 2, height + 2, width, chans), BF16),
                pltpu.VMEM((2, 2, height, width, chans), BF16),
                pltpu.VMEM(conv_kernels.shape, BF16),
                pltpu.VMEM((2, chans), F32),
                pltpu.VMEM((2, chans), F32),
                pltpu.VMEM((2, chans), F32),
                pltpu.VMEM((LAYERS, 2, chans), F32),
                pltpu.VMEM((LAYERS, LINE, 2, chans), F32),
                pltpu.VMEM((LAYERS, far, 2, chans), F32),
                pltpu.VMEM((2, 1, chans), F32),
                pltpu.VMEM((ROWS, 2, width, chans), F32),
                pltpu.VMEM((ROWS, 2, width + 16, chans), F32),
                pltpu.VMEM((ROWS, 2, width + 16, chans), F32),
                dma((n_frames,)),
                dma((LAYERS,)),
                dma((2,)),
                dma((2, height // CHUNK)),
                dma((2, height // CHUNK)),
                dma,
                dma((LAYERS,)),
                dma((LINE, 2)),
                dma((LAYERS, LINE)),
                dma((far,)),
                dma((LAYERS, far)),
            ],
            compiler_params=pltpu.CompilerParams(has_side_effects=True, vmem_limit_bytes=60 * 1024 * 1024),
            name="resblocks",
        )(latent, conv_kernels, conv_biases.reshape(row), gn_gammas.reshape(row), gn_betas.reshape(row))

    return jax.shard_map(local_fn, mesh=mesh, in_specs=(frame_spec, P(), P(), P(), P()), out_specs=frame_spec, check_vma=False)
```
